32 devices in a mesh: seq: 8 (over z, y), batch: 4 (over x, core).
Axes of the slice: x: 2, y: 2, z: 4, core: 2. Of those that a mesh axis runs over, the one named last changes fastest.
Arguments:
- queries: bfloat16 [4, 4096, 16, 128], P('batch', 'seq'), may hold values from -5 to 5
- keys: bfloat16 [4, 4096, 16, 128], P('batch', 'seq'), may hold values from -5 to 5
- values: bfloat16 [4, 4096, 16, 128], P('batch', 'seq'), may hold values from -5 to 5
- keep_count: int32 [4, 16, 32], P('batch'), may hold values from 0 to 128
- query_map: bfloat16 [16, 128, 8], replicated, may hold values from -0.5 to 0.5
- key_map: bfloat16 [16, 128, 8], replicated, may hold values from -0.5 to 0.5
- cotangent: bfloat16 [4, 4096, 16, 128], P('batch', 'seq'), may hold values from -5 to 5
Outputs:
- attended: bfloat16 [4, 4096, 16, 128], P('batch', 'seq')
- grad_query_map: float32 [16, 128, 8], replicated
- grad_key_map: float32 [16, 128, 8], replicated
The draws below stay inside these ranges and needn't reach their ends.
All inputs are finite; a program needn't handle non-finite values.
Results may differ from the reference program's by a relative error of at most 0.0035.
Values may be sent and summed in bfloat16 or wider, within the bound.
A program may use at most 128 MiB of HBM per device.

```python
import math
import jax
import jax.numpy as jnp
from jax import lax

HEADS = 16
DH = 128
RANK = 8
TILE = 128
WINDOW = 256
LEN = 4096
SEQS = 4
TILES = 32


def draw_queries(key, part):
    base = jax.random.truncated_normal(jax.random.fold_in(key, 1), -5.0, 5.0, (SEQS, LEN, HEADS, DH), jnp.float32)
    return base.astype(jnp.bfloat16)


def draw_keys(key, part):
    base = jax.random.truncated_normal(jax.random.fold_in(key, 2), -5.0, 5.0, (SEQS, LEN, HEADS, DH), jnp.float32)
    return base.astype(jnp.bfloat16)


def touch_ends(entries, key, least, top_value):
    longest = entries.shape.index(max(entries.shape))
    spots = []
    for shift in (0, 1):
        where = [jax.random.randint(jax.random.fold_in(key, axis), (), 0, length) for axis, length in enumerate(entries.shape)]
        where[longest] = (where[longest] + shift) % entries.shape[longest]
        spots.append(tuple(where))
    return entries.at[spots[0]].set(least).at[spots[1]].set(top_value)


def shard_levels(stream_key, dims, split, low, largest):
    factor_of, own = 1.0, jax.random.fold_in(stream_key, 6)
    for axis_at, parts in split:
        heights = jnp.exp(jax.random.uniform(jax.random.fold_in(own, axis_at), (parts,), jnp.float32, low / len(split), largest / len(split)))
        factor_of = factor_of * jnp.repeat(heights, dims[axis_at] // parts).reshape([-1 if axis == axis_at else 1 for axis in range(len(dims))])
    return factor_of


def centred(key, dims, scale, bound, split=(), kind=jnp.bfloat16):
    values = scale * jax.random.normal(key, dims, jnp.float32)
    if split:
        values = values * shard_levels(key, dims, split, -0.22, 0.18)
    return jnp.clip(values, -bound, bound).astype(kind)


def setup_inputs(seed: int = 0) -> dict:
    key_of = jax.random.split(jax.random.key(seed), 8)
    queries = draw_queries(jax.random.fold_in(key_of[7], 71), 0)
    keys = draw_keys(jax.random.fold_in(key_of[7], 71), 0)
    values = centred(key_of[2], (SEQS, LEN, HEADS, DH), 1.0, 5.0, ((0, 4), (1, 8)))
    keep_count = touch_ends(jax.random.randint(key_of[3], (SEQS, HEADS, TILES), 0, TILE + 1), jax.random.fold_in(key_of[3], 1), 0, TILE).astype(jnp.int32)
    query_map = centred(key_of[4], (HEADS, DH, RANK), DH ** -0.5, 0.5)
    key_map = centred(key_of[5], (HEADS, DH, RANK), DH ** -0.5, 0.5)
    cotangent = centred(key_of[6], (SEQS, LEN, HEADS, DH), 1.0, 5.0, ((0, 4), (1, 8)))
    return {"queries": queries, "keys": keys, "values": values, "keep_count": keep_count, "query_map": query_map, "key_map": key_map, "cotangent": cotangent}


HIGHEST = lax.Precision.HIGHEST
feature_shift = 1.5

def features(inputs, weights):
    pre_act = jnp.einsum('thd,hdr->thr', inputs.astype(jnp.float32), weights, precision=HIGHEST) - feature_shift
    return jax.nn.softplus(pre_act)

def shifted(array, offset):
    filler = jnp.zeros((offset,) + array.shape[1:], array.dtype)
    return jnp.concatenate([filler, array[:array.shape[0] - offset]], 0)

def exclusive(array):
    summed = jnp.cumsum(array, 0)
    return jnp.concatenate([jnp.zeros_like(array[:1]), summed[:-1]], 0)

def sparse_part(q_rows, k_rows, v_rows, kept):
    length, heads, width = q_rows.shape
    span = WINDOW // TILE
    scale = 1.0 / math.sqrt(width)
    filler = jnp.zeros((WINDOW, heads, width), k_rows.dtype)
    k_padded = jnp.concatenate([filler, k_rows], 0)
    v_padded = jnp.concatenate([filler, v_rows], 0)
    kept_padded = jnp.concatenate([jnp.zeros((WINDOW, heads), bool), kept], 0)

    def one_block(block):
        start = (block * WINDOW).astype(jnp.int32)
        q_block = lax.dynamic_slice_in_dim(q_rows, start, WINDOW, 0)
        k_block = lax.dynamic_slice_in_dim(k_padded, start, 2 * WINDOW, 0)
        v_block = lax.dynamic_slice_in_dim(v_padded, start, 2 * WINDOW, 0)
        kept_block = lax.dynamic_slice_in_dim(kept_padded, start, 2 * WINDOW, 0)
        q_pos = start + jnp.arange(WINDOW, dtype=jnp.int32)
        k_pos = start - WINDOW + jnp.arange(2 * WINDOW, dtype=jnp.int32)
        scores = jnp.einsum('thd,phd->htp', q_block.astype(jnp.float32), k_block.astype(jnp.float32)) * scale
        tile_gap = q_pos[:, None] // TILE - k_pos[None, :] // TILE
        causal = (k_pos[None, :] <= q_pos[:, None]) & (k_pos[None, :] >= 0) & (tile_gap < span)
        live_pairs = causal[None] & ((tile_gap == 0)[None] | kept_block.T[:, None, :])
        row_max = lax.optimization_barrier(jnp.max(jnp.where(live_pairs, scores, -jnp.inf), -1))
        weights = jnp.where(live_pairs, jnp.exp(scores - row_max[..., None]), 0.0)
        denom = lax.optimization_barrier(jnp.sum(weights, -1))
        numer = jnp.einsum('htp,phd->thd', weights.astype(jnp.bfloat16).astype(jnp.float32), v_block.astype(jnp.float32))
        return (numer, denom.T, row_max.T)
    numer, denom, row_max = lax.map(one_block, jnp.arange(length // WINDOW, dtype=jnp.int32))
    return (numer.reshape(length, heads, width), denom.reshape(length, heads), row_max.reshape(length, heads))

def reference(queries, keys, values, keep_count, query_map, key_map, cotangent):
    query_weights = query_map.astype(jnp.float32)
    key_weights = key_map.astype(jnp.float32)
    span = WINDOW // TILE

    def one_sequence(inputs):
        q_rows, k_rows, v_rows, counts, cot_rows = inputs
        length, heads, width = q_rows.shape
        tiles = length // TILE
        within = jnp.arange(length, dtype=jnp.int32) % TILE
        kept = within[:, None] < jnp.repeat(counts, TILE, axis=1).T
        numer, denom, row_max = sparse_part(q_rows, k_rows, v_rows, kept)
        decay = jnp.exp(-row_max)
        v_tiles = v_rows.astype(jnp.float32).reshape(tiles, TILE, heads, width)
        evicted = (1 - kept.astype(jnp.float32)).reshape(tiles, TILE, heads, 1)

        def linear(q_weights, k_weights):
            feat_q = features(q_rows, q_weights).reshape(tiles, TILE, heads, RANK)
            feat_k = features(k_rows, k_weights).reshape(tiles, TILE, heads, RANK)
            all_state = jnp.einsum('nthr,nthd->nhrd', feat_k, v_tiles, precision=HIGHEST)
            all_norm = lax.optimization_barrier(jnp.sum(feat_k, 1))
            ev_feat = feat_k * evicted
            ev_state = jnp.einsum('nthr,nthd->nhrd', ev_feat, v_tiles, precision=HIGHEST)
            ev_norm = lax.optimization_barrier(jnp.sum(ev_feat, 1))
            state = shifted(exclusive(all_state), span - 1)
            norm = shifted(exclusive(all_norm), span - 1)
            for offset in range(1, span):
                state = state + shifted(ev_state, offset)
                norm = norm + shifted(ev_norm, offset)
            kernel_num = jnp.einsum('nthr,nhrd->nthd', feat_q, state, precision=HIGHEST).reshape(length, heads, width)
            kernel_den = jnp.einsum('nthr,nhr->nth', feat_q, norm, precision=HIGHEST).reshape(length, heads)
            return (numer + decay[..., None] * kernel_num) / (denom + decay * kernel_den)[..., None]
        out, pull_back = jax.vjp(linear, query_weights, key_weights)
        grad_q, grad_k = pull_back(cot_rows.astype(jnp.float32))
        return (out.astype(jnp.bfloat16), grad_q, grad_k)
    attended, grad_q, grad_k = lax.map(one_sequence, (queries, keys, values, keep_count, cotangent))
    return (attended, lax.optimization_barrier(jnp.sum(grad_q, 0)), lax.optimization_barrier(jnp.sum(grad_k, 0)))
```

```python
import functools
import math

import jax
import jax.numpy as jnp
from jax import lax
from jax.experimental import pallas as pl
from jax.experimental.pallas import tpu as pltpu
from jax.sharding import PartitionSpec as P

TILE = 128
SHIFT = 1.5
LOG2E = 1.0 / math.log(2.0)
MASKED = -1e30
F32 = jnp.float32
BF16 = jnp.bfloat16
VMEM_LIMIT = 56 * 1024 * 1024


def dot_nt(a, b):
    return lax.dot_general(a, b, (((1,), (1,)), ((), ())), preferred_element_type=F32)


def dot_nn(a, b):
    return lax.dot_general(a, b, (((1,), (0,)), ((), ())), preferred_element_type=F32)


def dot_tn(a, b):
    return lax.dot_general(a, b, (((0,), (0,)), ((), ())), preferred_element_type=F32)


def by_head(x):
    return jnp.swapaxes(x, 0, 1)


def softplus(x):
    return jnp.maximum(x, 0.0) + jnp.log1p(jnp.exp(-jnp.abs(x)))


def sigmoid(x):
    return 1.0 / (1.0 + jnp.exp(-x))


def halves(x):
    top = x.astype(BF16)
    return top, (x - top.astype(F32)).astype(BF16)


def split_dot(dot, x, y):
    rows = x.shape[0]
    both = dot(jnp.concatenate(halves(x), 0), y)
    return both[:rows] + both[rows:]


def with_ones(v):
    return jnp.concatenate([v, jnp.ones(v.shape, v.dtype)], 1)


def state_kernel(k_ref, v_ref, wk_ref, kh_ref, vh_ref, total_ref, acc_ref):
    step = pl.program_id(0)
    heads = wk_ref.shape[0]
    kh_ref[...] = by_head(k_ref[...])
    vh_ref[...] = by_head(v_ref[...])

    @pl.when(step == 0)
    def _():
        acc_ref[...] = jnp.zeros_like(acc_ref)

    def one_head(h, carry):
        feat = softplus(dot_nt(wk_ref[h], kh_ref[h]) - SHIFT)
        acc_ref[h] += split_dot(dot_nn, feat, with_ones(vh_ref[h]))
        return carry

    lax.fori_loop(0, heads, one_head, 0, unroll=4)

    @pl.when(step == pl.num_programs(0) - 1)
    def _():
        total_ref[...] = acc_ref[...]


def local_states(k_rows, v_rows, wk):
    tokens, heads, width = k_rows.shape
    rank = wk.shape[1]
    row_spec = pl.BlockSpec((TILE, heads, width), lambda n: (n, 0, 0))
    head_spec = pl.BlockSpec((heads, TILE, width), lambda n: (0, n, 0))
    return pl.pallas_call(
        state_kernel,
        name="local_states",
        grid=(tokens // TILE,),
        in_specs=[row_spec, row_spec, pl.BlockSpec(wk.shape, lambda n: (0, 0, 0))],
        out_specs=[head_spec, head_spec, pl.BlockSpec((heads, rank, 2 * width), lambda n: (0, 0, 0))],
        out_shape=[
            jax.ShapeDtypeStruct((heads, tokens, width), BF16),
            jax.ShapeDtypeStruct((heads, tokens, width), BF16),
            jax.ShapeDtypeStruct((heads, rank, 2 * width), F32),
        ],
        scratch_shapes=[pltpu.VMEM((heads, rank, 2 * width), F32)],
        compiler_params=pltpu.CompilerParams(vmem_limit_bytes=VMEM_LIMIT),
        cost_estimate=pl.CostEstimate(flops=10**9, bytes_accessed=8 * 2**20, transcendentals=10**6),
    )(k_rows, v_rows, wk)


def main_kernel(
    first, halo, counts_ref, where_ref, q_ref, k_ref, v_ref, kp_ref, vp_ref, c_ref, wq_ref, wk_ref,
    states_ref, out_ref, ds_ref, gq_ref, gk_ref, qh, ch, oh, kph, vph, run,
):
    step = pl.program_id(0)
    heads = wq_ref.shape[0]
    peers = states_ref.shape[0]
    width = q_ref.shape[2]
    me = where_ref[0]
    tiles_dev = where_ref[1]
    factor = LOG2E / math.sqrt(width)
    qh[...] = by_head(q_ref[...])
    ch[...] = by_head(c_ref[...])
    if halo:
        kph[...] = by_head(kp_ref[...])
        vph[...] = by_head(vp_ref[...])
    prev_k = kph if halo else kp_ref
    prev_v = vph if halo else vp_ref

    @pl.when(step == 0)
    def _():
        gq_ref[...] = jnp.zeros_like(gq_ref)
        gk_ref[...] = jnp.zeros_like(gk_ref)
        before = jnp.zeros(run.shape, F32)
        for peer in range(peers):
            before += jnp.where(peer < me, states_ref[peer].astype(F32), 0.0)
        run[...] = before

    tile = me * tiles_dev + first + step
    lane = lax.broadcasted_iota(jnp.int32, (1, TILE), 1)
    row = lax.broadcasted_iota(jnp.int32, (TILE, TILE), 0)
    col = lax.broadcasted_iota(jnp.int32, (TILE, TILE), 1)
    causal = col <= row

    def one_head(h, carry):
        q, c = qh[h], ch[h]
        k, v = k_ref[h], v_ref[h]
        kp, vp = prev_k[h], prev_v[h]
        count = jnp.where(tile > 0, counts_ref[h, jnp.maximum(tile - 1, 0)], 0)
        kept = lane < count
        kept_f = kept.astype(F32)
        pre_p = dot_nt(wk_ref[h], kp) - SHIFT
        feat_p = softplus(pre_p)
        vp_ext = with_ones(vp)
        rank = feat_p.shape[0]
        both = split_dot(dot_nn, jnp.concatenate([feat_p, feat_p * kept_f], 0), vp_ext)
        if halo:
            state = run[h] - both[rank:]
        else:
            total = run[h] + both[:rank]
            run[h] = total
            state = total - both[rank:]
        own = jnp.where(causal, dot_nt(q, k), MASKED)
        old = jnp.where(kept, dot_nt(q, kp), MASKED)
        top = jnp.max(jnp.maximum(own, old), 1, keepdims=True) * factor
        p_own = jnp.exp2(own * factor - top).astype(BF16)
        p_old = jnp.exp2(old * factor - top).astype(BF16)
        numer = dot_nn(p_own, with_ones(v)) + dot_nn(p_old, vp_ext)
        decay = jnp.exp2(-top)
        pre_q = dot_nt(wq_ref[h], q) - SHIFT
        feat_q = softplus(pre_q)
        fq_top, fq_low = halves(feat_q)
        st_top, st_low = halves(state)
        kernel = dot_tn(jnp.concatenate([fq_top, fq_low, fq_top], 0), jnp.concatenate([st_top, st_top, st_low], 0))
        full = numer + decay * kernel
        inv = 1.0 / full[:, width:]
        out = full[:, :width] * inv
        oh[h] = out.astype(BF16)
        gn = decay * (c.astype(F32) * inv)
        g_ext = jnp.concatenate([gn, gn * out], 1).astype(BF16)
        signed = jnp.concatenate([state[:, :width], -state[:, width:]], 1)
        dpre_q = split_dot(dot_nt, signed, g_ext) * sigmoid(pre_q)
        gq_ref[h] += split_dot(dot_nn, dpre_q, q)
        ds = split_dot(dot_nn, feat_q, g_ext)
        ds_ref[0, h] = ds
        dn = -jnp.sum(ds[:, width:], 1, keepdims=True)
        dfk = split_dot(dot_nt, ds[:, :width], vp) + dn
        dpre_k = -kept_f * dfk * sigmoid(pre_p)
        gk_ref[h] += split_dot(dot_nn, dpre_k, kp)
        return carry

    lax.fori_loop(0, heads, one_head, 0, unroll=4)
    out_ref[...] = by_head(oh[...])


def attend(first, steps, halo, counts, where, q_rows, kh, vh, kp, vp, cot, wq, wk, states):
    tokens, heads, width = q_rows.shape
    rank = wq.shape[1]
    row_spec = pl.BlockSpec((TILE, heads, width), lambda n: (n + first, 0, 0))
    head_spec = pl.BlockSpec((heads, TILE, width), lambda n: (0, n + first, 0))
    if halo:
        prev_spec = pl.BlockSpec((TILE, heads, width), lambda n: (0, 0, 0))
    else:
        prev_spec = pl.BlockSpec((heads, TILE, width), lambda n: (0, n + first - 1, 0))
    whole = pl.BlockSpec((heads, rank, width), lambda n: (0, 0, 0))
    smem = pl.BlockSpec(memory_space=pltpu.SMEM)
    tile_scratch = pltpu.VMEM((heads, TILE, width), BF16)
    return pl.pallas_call(
        functools.partial(main_kernel, first, halo),
        name="attend_first" if halo else "attend_rest",
        grid=(steps,),
        in_specs=[
            smem, smem, row_spec, head_spec, head_spec, prev_spec, prev_spec, row_spec, whole, whole,
            pl.BlockSpec(states.shape, lambda n: (0, 0, 0, 0)),
        ],
        out_specs=[
            pl.BlockSpec((TILE, heads, width), lambda n: (n, 0, 0)),
            pl.BlockSpec((1, heads, rank, 2 * width), lambda n: (n, 0, 0, 0)),
            whole,
            whole,
        ],
        out_shape=[
            jax.ShapeDtypeStruct((steps * TILE, heads, width), BF16),
            jax.ShapeDtypeStruct((steps, heads, rank, 2 * width), F32),
            jax.ShapeDtypeStruct((heads, rank, width), F32),
            jax.ShapeDtypeStruct((heads, rank, width), F32),
        ],
        scratch_shapes=[tile_scratch] * 5 + [pltpu.VMEM((heads, rank, 2 * width), F32)],
        compiler_params=pltpu.CompilerParams(vmem_limit_bytes=VMEM_LIMIT),
        cost_estimate=pl.CostEstimate(flops=10**9 * steps, bytes_accessed=steps * 4 * 2**20, transcendentals=10**6),
    )(counts, where, q_rows, kh, vh, kp, vp, cot, wq, wk, states)


def key_kernel(where_ref, kh_ref, vh_ref, wk_ref, ds0_ref, ds1_ref, after_ref, gk_ref):
    group, tokens, width = kh_ref.shape
    tiles = tokens // TILE
    me = where_ref[0]
    for h in range(group):
        later = jnp.zeros(ds0_ref.shape[2:], F32)
        for peer in range(after_ref.shape[0]):
            later += jnp.where(peer > me, after_ref[peer, h].astype(F32), 0.0)
        pre = dot_nt(wk_ref[h], kh_ref[h]) - SHIFT
        pieces = [None] * tiles
        for n in reversed(range(tiles)):
            dn = -jnp.sum(later[:, width:], 1, keepdims=True)
            pieces[n] = split_dot(dot_nt, later[:, :width], vh_ref[h, n * TILE : (n + 1) * TILE]) + dn
            if n:
                later += ds1_ref[n - 1, h]
        grad = jnp.concatenate(pieces, 1) * sigmoid(pre)
        gk_ref[h] = split_dot(dot_nn, grad, kh_ref[h])


def key_grads(where, kh, vh, wk, ds0, ds1, after):
    heads, tokens, width = kh.shape
    rank = wk.shape[1]
    group = 4
    head_spec = pl.BlockSpec((group, tokens, width), lambda n: (n, 0, 0))
    whole = pl.BlockSpec((group, rank, width), lambda n: (n, 0, 0))

    def four(a):
        return pl.BlockSpec((a.shape[0], group) + a.shape[2:], lambda n: (0, n, 0, 0))

    return pl.pallas_call(
        key_kernel,
        name="key_grads",
        grid=(heads // group,),
        in_specs=[
            pl.BlockSpec(memory_space=pltpu.SMEM), head_spec, head_spec, whole, four(ds0), four(ds1), four(after),
        ],
        out_specs=whole,
        out_shape=jax.ShapeDtypeStruct((heads, rank, width), F32),
        compiler_params=pltpu.CompilerParams(vmem_limit_bytes=VMEM_LIMIT),
        cost_estimate=pl.CostEstimate(flops=10**9, bytes_accessed=8 * 2**20, transcendentals=10**6),
    )(where, kh, vh, wk, ds0, ds1, after)


def body(queries, keys, values, keep_count, query_map, key_map, cotangent):
    q_rows, k_rows, v_rows, cot = queries[0], keys[0], values[0], cotangent[0]
    counts = keep_count[0]
    tokens = q_rows.shape[0]
    tiles = tokens // TILE
    peers = lax.axis_size("seq")
    me = lax.axis_index("seq")
    where = jnp.stack([me, jnp.int32(tiles)]).astype(jnp.int32)
    ring = [(a, a + 1) for a in range(peers - 1)]
    kp, vp = lax.ppermute((k_rows[tokens - TILE :], v_rows[tokens - TILE :]), "seq", ring)
    wq = jnp.swapaxes(query_map, 1, 2)
    wk = jnp.swapaxes(key_map, 1, 2)
    kh, vh, total = local_states(k_rows, v_rows, wk)
    states = lax.all_gather(total, "seq")
    rest = attend(1, tiles - 1, False, counts, where, q_rows, kh, vh, kh, vh, cot, wq, wk, states)
    head = attend(0, 1, True, counts, where, q_rows, kh, vh, kp, vp, cot, wq, wk, states)
    own = head[1][0] + jnp.sum(rest[1], 0)
    after = lax.all_gather(own, "seq")
    gk = key_grads(where, kh, vh, wk, head[1], rest[1], after)
    grads = jnp.stack([head[2] + rest[2], head[3] + rest[3] + gk])
    grads = lax.psum(grads, ("seq", "batch"))
    grads = jnp.swapaxes(grads, 2, 3)
    out = jnp.concatenate([head[0], rest[0]], 0)
    return out[None], grads[0], grads[1]


def solution(mesh):
    placed = (
        P("batch", "seq", None, None),
        P("batch", "seq", None, None),
        P("batch", "seq", None, None),
        P("batch", None, None),
        P(),
        P(),
        P("batch", "seq", None, None),
    )
    return jax.shard_map(
        body,
        mesh=mesh,
        in_specs=placed,
        out_specs=(P("batch", "seq", None, None), P(), P()),
        check_vma=False,
    )
```

```python
import functools
import math

import jax
import jax.numpy as jnp
from jax import lax
from jax.experimental import pallas as pl
from jax.experimental.pallas import tpu as pltpu
from jax.sharding import PartitionSpec as P

TILE = 128
SHIFT = 1.5
LOG2E = 1.0 / math.log(2.0)
MASKED = -1e30
F32 = jnp.float32
BF16 = jnp.bfloat16
GROUP = 4
VMEM_LIMIT = 56 * 1024 * 1024


def dot_nt(a, b):
    return lax.dot_general(a, b, (((1,), (1,)), ((), ())), preferred_element_type=F32)


def dot_nn(a, b):
    return lax.dot_general(a, b, (((1,), (0,)), ((), ())), preferred_element_type=F32)


def dot_tn(a, b):
    return lax.dot_general(a, b, (((0,), (0,)), ((), ())), preferred_element_type=F32)


def by_head(x):
    return jnp.swapaxes(x, 0, 1)


def softplus(x):
    return jnp.maximum(x, 0.0) + jnp.log1p(jnp.exp(-jnp.abs(x)))


def sigmoid(x):
    return 1.0 / (1.0 + jnp.exp(-x))


def halves(x):
    top = x.astype(BF16)
    return top, (x - top.astype(F32)).astype(BF16)


def split_dot(dot, x, y):
    rows = x.shape[0]
    both = dot(jnp.concatenate(halves(x), 0), y)
    return both[:rows] + both[rows:]


def with_ones(v):
    return jnp.concatenate([v, jnp.ones(v.shape, v.dtype)], 1)


def state_kernel(k_ref, v_ref, wk_ref, kh_ref, vh_ref, total_ref, acc_ref):
    step = pl.program_id(0)
    heads = wk_ref.shape[0]
    kh_ref[...] = by_head(k_ref[...])
    vh_ref[...] = by_head(v_ref[...])

    @pl.when(step == 0)
    def _():
        acc_ref[...] = jnp.zeros_like(acc_ref)

    pre = jnp.stack([dot_nt(wk_ref[h], kh_ref[h]) for h in range(heads)], 0)
    feat = softplus(pre - SHIFT)
    for h in range(heads):
        acc_ref[h] += split_dot(dot_nn, feat[h], with_ones(vh_ref[h]))

    @pl.when(step == pl.num_programs(0) - 1)
    def _():
        total_ref[...] = acc_ref[...]


def local_states(k_rows, v_rows, wk):
    tokens, heads, width = k_rows.shape
    rank = wk.shape[1]
    row_spec = pl.BlockSpec((TILE, heads, width), lambda n: (n, 0, 0))
    head_spec = pl.BlockSpec((heads, TILE, width), lambda n: (0, n, 0))
    return pl.pallas_call(
        state_kernel,
        name="local_states",
        grid=(tokens // TILE,),
        in_specs=[row_spec, row_spec, pl.BlockSpec(wk.shape, lambda n: (0, 0, 0))],
        out_specs=[head_spec, head_spec, pl.BlockSpec((heads, rank, 2 * width), lambda n: (0, 0, 0))],
        out_shape=[
            jax.ShapeDtypeStruct((heads, tokens, width), BF16),
            jax.ShapeDtypeStruct((heads, tokens, width), BF16),
            jax.ShapeDtypeStruct((heads, rank, 2 * width), F32),
        ],
        scratch_shapes=[pltpu.VMEM((heads, rank, 2 * width), F32)],
        compiler_params=pltpu.CompilerParams(vmem_limit_bytes=VMEM_LIMIT),
        cost_estimate=pl.CostEstimate(flops=10**9, bytes_accessed=8 * 2**20, transcendentals=10**6),
    )(k_rows, v_rows, wk)


def main_kernel(
    first, halo, counts_ref, where_ref, q_ref, k_ref, v_ref, kp_ref, vp_ref, c_ref, wq_ref, wk_ref,
    states_ref, out_ref, ds_ref, gq_ref, gk_ref, qh, ch, oh, kph, vph, run,
):
    step = pl.program_id(0)
    heads = wq_ref.shape[0]
    width = q_ref.shape[2]
    me = where_ref[0]
    tiles_dev = where_ref[1]
    factor = LOG2E / math.sqrt(width)
    qh[...] = by_head(q_ref[...])
    ch[...] = by_head(c_ref[...])
    if halo:
        kph[...] = by_head(kp_ref[...])
        vph[...] = by_head(vp_ref[...])
    prev_k = kph if halo else kp_ref
    prev_v = vph if halo else vp_ref

    @pl.when(step == 0)
    def _():
        gq_ref[...] = jnp.zeros_like(gq_ref)
        gk_ref[...] = jnp.zeros_like(gk_ref)
        run[...] = states_ref[...]

    tile = me * tiles_dev + first + step
    lane = lax.broadcasted_iota(jnp.int32, (1, TILE), 1)
    row = lax.broadcasted_iota(jnp.int32, (TILE, TILE), 0)
    col = lax.broadcasted_iota(jnp.int32, (TILE, TILE), 1)
    causal = col <= row

    def some_heads(g, carry):
        hs = [g * GROUP + i for i in range(GROUP)]
        each = range(GROUP)
        qs, ks, vs = [qh[h] for h in hs], [k_ref[h] for h in hs], [v_ref[h] for h in hs]
        kps, vps = [prev_k[h] for h in hs], [prev_v[h] for h in hs]
        own_raw = [dot_nt(qs[i], ks[i]) for i in each]
        old_raw = [dot_nt(qs[i], kps[i]) for i in each]
        pre_p = [dot_nt(wk_ref[hs[i]], kps[i]) - SHIFT for i in each]
        pre_q = [dot_nt(wq_ref[hs[i]], qs[i]) - SHIFT for i in each]
        counts = [jnp.where(tile > 0, counts_ref[h, jnp.maximum(tile - 1, 0)], 0) for h in hs]
        kept = [lane < count for count in counts]
        kept_f = [keep.astype(F32) for keep in kept]
        own = [jnp.where(causal, own_raw[i], MASKED) for i in each]
        old = [jnp.where(kept[i], old_raw[i], MASKED) for i in each]
        top = [jnp.max(jnp.maximum(own[i], old[i]), 1, keepdims=True) * factor for i in each]
        feat_p = [softplus(pre) for pre in pre_p]
        feat_q = [softplus(pre) for pre in pre_q]
        both = [
            split_dot(dot_nn, jnp.concatenate([feat_p[i], feat_p[i] * kept_f[i]], 0), with_ones(vps[i])) for i in each
        ]
        state = []
        for i in each:
            rank = feat_p[i].shape[0]
            total = run[hs[i]]
            if not halo:
                total += both[i][:rank]
                run[hs[i]] = total
            state.append(total - both[i][rank:])
        p_own = [jnp.exp2(own[i] * factor - top[i]).astype(BF16) for i in each]
        p_old = [jnp.exp2(old[i] * factor - top[i]).astype(BF16) for i in each]
        numer = [dot_nn(p_own[i], with_ones(vs[i])) + dot_nn(p_old[i], with_ones(vps[i])) for i in each]
        decay = [jnp.exp2(-t) for t in top]
        kernel = []
        for i in each:
            fq_top, fq_low = halves(feat_q[i])
            st_top, st_low = halves(state[i])
            kernel.append(
                dot_tn(jnp.concatenate([fq_top, fq_low, fq_top], 0), jnp.concatenate([st_top, st_top, st_low], 0))
            )
        g_ext = []
        for i in each:
            full = numer[i] + decay[i] * kernel[i]
            inv = 1.0 / full[:, width:]
            out = full[:, :width] * inv
            oh[hs[i]] = out.astype(BF16)
            gn = decay[i] * (ch[hs[i]].astype(F32) * inv)
            g_ext.append(jnp.concatenate([gn, gn * out], 1).astype(BF16))
        signed = [jnp.concatenate([st[:, :width], -st[:, width:]], 1) for st in state]
        d_fq = [split_dot(dot_nt, signed[i], g_ext[i]) for i in each]
        ds = [split_dot(dot_nn, feat_q[i], g_ext[i]) for i in each]
        dpre_q = [d_fq[i] * sigmoid(pre_q[i]) for i in each]
        d_fk = [
            split_dot(dot_nt, ds[i][:, :width], vps[i]) - jnp.sum(ds[i][:, width:], 1, keepdims=True) for i in each
        ]
        dpre_k = [-kept_f[i] * d_fk[i] * sigmoid(pre_p[i]) for i in each]
        gq = [split_dot(dot_nn, dpre_q[i], qs[i]) for i in each]
        gk = [split_dot(dot_nn, dpre_k[i], kps[i]) for i in each]
        for i in each:
            ds_ref[0, hs[i]] = ds[i]
            gq_ref[hs[i]] += gq[i]
            gk_ref[hs[i]] += gk[i]
        return carry

    lax.fori_loop(0, heads // GROUP, some_heads, 0)
    out_ref[...] = by_head(oh[...])


def attend(first, steps, halo, counts, where, q_rows, kh, vh, kp, vp, cot, wq, wk, states):
    tokens, heads, width = q_rows.shape
    rank = wq.shape[1]
    row_spec = pl.BlockSpec((TILE, heads, width), lambda n: (n + first, 0, 0))
    head_spec = pl.BlockSpec((heads, TILE, width), lambda n: (0, n + first, 0))
    if halo:
        prev_spec = pl.BlockSpec((TILE, heads, width), lambda n: (0, 0, 0))
    else:
        prev_spec = pl.BlockSpec((heads, TILE, width), lambda n: (0, n + first - 1, 0))
    whole = pl.BlockSpec((heads, rank, width), lambda n: (0, 0, 0))
    smem = pl.BlockSpec(memory_space=pltpu.SMEM)
    tile_scratch = pltpu.VMEM((heads, TILE, width), BF16)
    return pl.pallas_call(
        functools.partial(main_kernel, first, halo),
        name="attend_first" if halo else "attend_rest",
        grid=(steps,),
        in_specs=[
            smem, smem, row_spec, head_spec, head_spec, prev_spec, prev_spec, row_spec, whole, whole,
            pl.BlockSpec(states.shape, lambda n: (0, 0, 0)),
        ],
        out_specs=[
            pl.BlockSpec((TILE, heads, width), lambda n: (n, 0, 0)),
            pl.BlockSpec((1, heads, rank, 2 * width), lambda n: (n, 0, 0, 0)),
            whole,
            whole,
        ],
        out_shape=[
            jax.ShapeDtypeStruct((steps * TILE, heads, width), BF16),
            jax.ShapeDtypeStruct((steps, heads, rank, 2 * width), F32),
            jax.ShapeDtypeStruct((heads, rank, width), F32),
            jax.ShapeDtypeStruct((heads, rank, width), F32),
        ],
        scratch_shapes=[tile_scratch] * 5 + [pltpu.VMEM((heads, rank, 2 * width), F32)],
        compiler_params=pltpu.CompilerParams(vmem_limit_bytes=VMEM_LIMIT),
        cost_estimate=pl.CostEstimate(flops=10**9 * steps, bytes_accessed=steps * 4 * 2**20, transcendentals=10**6),
    )(counts, where, q_rows, kh, vh, kp, vp, cot, wq, wk, states)


def key_kernel(kh_ref, vh_ref, wk_ref, ds1_ref, after_ref, gk_ref):
    group, tokens, width = kh_ref.shape
    tiles = tokens // TILE
    each = range(group)
    pre = [dot_nt(wk_ref[h], kh_ref[h]) - SHIFT for h in each]
    grads = []
    for h in each:
        later = after_ref[h][:, :width]
        norm = after_ref[h][:, width:]
        pieces = [None] * tiles
        for n in reversed(range(tiles)):
            pieces[n] = split_dot(dot_nt, later, vh_ref[h, n * TILE : (n + 1) * TILE]) + norm
            if n:
                later += ds1_ref[n - 1, h][:, :width]
                norm -= jnp.sum(ds1_ref[n - 1, h][:, width:], 1, keepdims=True)
        grads.append(jnp.concatenate(pieces, 1))
    for h in each:
        gk_ref[h] = split_dot(dot_nn, grads[h] * sigmoid(pre[h]), kh_ref[h])


def flat_id(axes):
    index, count = 0, 1
    for axis in axes:
        index = index * lax.axis_size(axis) + lax.axis_index(axis)
        count *= lax.axis_size(axis)
    return index, count


def place(flat, axes):
    where = {}
    for axis in reversed(axes):
        size = lax.axis_size(axis)
        where[axis] = lax.rem(flat, size)
        flat = flat // size
    return where


def greet(count, me, axes):
    barrier = pltpu.get_barrier_semaphore()

    def hello(i, carry):
        pl.semaphore_signal(
            barrier, inc=1, device_id=place(lax.rem(me + i, count), axes), device_id_type=pl.DeviceIdType.MESH
        )
        return carry

    lax.fori_loop(1, count, hello, 0)
    return barrier


def others_kernel(axis, later, *refs):
    parts, (out_ref, mine, slots, send_sem, recv_sem) = refs[:-5], refs[-5:]
    heads, _, twice = out_ref.shape
    width = twice // 2
    axes = (axis,)
    me, count = flat_id(axes)
    barrier = greet(count, me, axes)
    lane = lax.broadcasted_iota(jnp.int32, (1, width), 1)
    packed = jnp.zeros(mine.shape[1:], F32)
    for h in range(heads):
        own = sum(part[n, h] for part in parts for n in range(part.shape[0]))
        mine[h] = own[:, :width]
        norm = -jnp.sum(own[:, width:], 1, keepdims=True) if later else own[:, width:]
        packed = jnp.where(lane == h, norm, packed)
    mine[heads] = packed
    pl.semaphore_wait(barrier, count - 1)

    def copy(sender, target):
        return pltpu.make_async_remote_copy(
            src_ref=mine,
            dst_ref=slots.at[sender],
            send_sem=send_sem.at[target],
            recv_sem=recv_sem.at[sender],
            device_id=place(target, axes),
            device_id_type=pl.DeviceIdType.MESH,
        )

    slots[me] = jnp.zeros(mine.shape, F32)
    if later:
        first_to, end_to, first_from, end_from = 0, me, me + 1, count
    else:
        first_to, end_to, first_from, end_from = me + 1, count, 0, me

    def send(p, carry):
        copy(me, p).start()
        return carry

    def sent(p, carry):
        copy(me, p).wait_send()
        return carry

    def received(p, total):
        copy(p, lax.rem(me + 1, count)).wait_recv()
        return total + slots[p]

    lax.fori_loop(first_to, end_to, send, 0)
    total = lax.fori_loop(first_from, end_from, received, jnp.zeros(mine.shape, F32))
    lax.fori_loop(first_to, end_to, sent, 0)
    for h in range(heads):
        norm = jnp.sum(jnp.where(lane == h, total[heads], 0.0), 1, keepdims=True)
        out_ref[h] = jnp.concatenate([total[h], jnp.broadcast_to(norm, total[h].shape)], 1)


def sum_of_others(parts, axis, later, collective_id):
    heads, rank, twice = parts[0].shape[1:]
    count = lax.axis_size(axis)
    block = (heads + 1, rank, twice // 2)
    vmem = pl.BlockSpec(memory_space=pltpu.VMEM)
    return pl.pallas_call(
        functools.partial(others_kernel, axis, later),
        name="later_grads" if later else "earlier_states",
        in_specs=[vmem] * len(parts),
        out_specs=vmem,
        out_shape=jax.ShapeDtypeStruct((heads, rank, twice), F32),
        scratch_shapes=[
            pltpu.VMEM(block, F32),
            pltpu.VMEM((count,) + block, F32),
            pltpu.SemaphoreType.DMA((count,)),
            pltpu.SemaphoreType.DMA((count,)),
        ],
        compiler_params=pltpu.CompilerParams(
            collective_id=collective_id, has_side_effects=True, vmem_limit_bytes=VMEM_LIMIT
        ),
        cost_estimate=pl.CostEstimate(flops=10**7, bytes_accessed=2**20, transcendentals=0),
    )(*parts)


def reduce_kernel(axes, gq0, gq1, gk0, gk1, gk2, out_ref, mine, slots, done, out_sem, in_sem, back_sem, res_sem):
    heads = gq0.shape[0]
    chunks = 2 * heads
    me, count = flat_id(axes)
    owners = min(count, chunks)
    stride, per = count // owners, chunks // owners
    barrier = greet(count, me, axes)
    mine[:heads] = gq0[...] + gq1[...]
    mine[heads:] = gk0[...] + gk1[...] + gk2[...]
    pl.semaphore_wait(barrier, count - 1)
    owner = lax.rem(me, stride) == 0
    part = me // stride

    def to_owner(o, sender):
        return pltpu.make_async_remote_copy(
            src_ref=mine.at[pl.ds(o * per, per)],
            dst_ref=slots.at[sender],
            send_sem=out_sem.at[o],
            recv_sem=in_sem.at[sender],
            device_id=place(o * stride, axes),
            device_id_type=pl.DeviceIdType.MESH,
        )

    def to_all(o, target):
        return pltpu.make_async_remote_copy(
            src_ref=done.at[pl.ds(o * per, per)],
            dst_ref=done.at[pl.ds(o * per, per)],
            send_sem=back_sem.at[target],
            recv_sem=res_sem.at[o],
            device_id=place(target, axes),
            device_id_type=pl.DeviceIdType.MESH,
        )

    def over_owners(act):
        def step(i, carry):
            o = lax.rem(part + i, owners)

            @pl.when(o * stride != me)
            def _():
                act(o)

            return carry

        lax.fori_loop(0, owners, step, 0)

    over_owners(lambda o: to_owner(o, me).start())

    @pl.when(owner)
    def _():
        def arrived(i, total):
            sender = lax.rem(me + i, count)
            to_owner(part, sender).wait_recv()
            return total + slots[sender]

        done[pl.ds(part * per, per)] = lax.fori_loop(1, count, arrived, mine[pl.ds(part * per, per)])

        def send(i, carry):
            to_all(part, lax.rem(me + i, count)).start()
            return carry

        lax.fori_loop(1, count, send, 0)

    over_owners(lambda o: to_owner(o, me).wait_send())
    over_owners(lambda o: to_all(o, lax.rem(me + 1, count)).wait_recv())

    @pl.when(owner)
    def _():
        def sent(i, carry):
            to_all(part, lax.rem(me + i, count)).wait_send()
            return carry

        lax.fori_loop(1, count, sent, 0)

    out_ref[...] = done[...]


def sum_over_all(grads, axes):
    heads, rank, width = grads[0].shape
    count = math.prod(lax.axis_size(axis) for axis in axes)
    owners = min(count, 2 * heads)
    per = 2 * heads // owners
    vmem = pl.BlockSpec(memory_space=pltpu.VMEM)
    whole = (2 * heads, rank, width)
    return pl.pallas_call(
        functools.partial(reduce_kernel, axes),
        name="sum_grads",
        in_specs=[vmem] * len(grads),
        out_specs=vmem,
        out_shape=jax.ShapeDtypeStruct(whole, F32),
        scratch_shapes=[
            pltpu.VMEM(whole, F32),
            pltpu.VMEM((count, per, rank, width), F32),
            pltpu.VMEM(whole, F32),
            pltpu.SemaphoreType.DMA((owners,)),
            pltpu.SemaphoreType.DMA((count,)),
            pltpu.SemaphoreType.DMA((count,)),
            pltpu.SemaphoreType.DMA((owners,)),
        ],
        compiler_params=pltpu.CompilerParams(collective_id=2, has_side_effects=True, vmem_limit_bytes=VMEM_LIMIT),
        cost_estimate=pl.CostEstimate(flops=10**7, bytes_accessed=2**20, transcendentals=0),
    )(*grads)


def key_grads(kh, vh, wk, ds1, after):
    heads, tokens, width = kh.shape
    rank = wk.shape[1]
    group = 4
    head_spec = pl.BlockSpec((group, tokens, width), lambda n: (n, 0, 0))
    whole = pl.BlockSpec((group, rank, width), lambda n: (n, 0, 0))
    four = pl.BlockSpec((ds1.shape[0], group, rank, 2 * width), lambda n: (0, n, 0, 0))

    return pl.pallas_call(
        key_kernel,
        name="key_grads",
        grid=(heads // group,),
        in_specs=[
            head_spec, head_spec, whole, four, pl.BlockSpec((group, rank, 2 * width), lambda n: (n, 0, 0)),
        ],
        out_specs=whole,
        out_shape=jax.ShapeDtypeStruct((heads, rank, width), F32),
        compiler_params=pltpu.CompilerParams(vmem_limit_bytes=VMEM_LIMIT),
        cost_estimate=pl.CostEstimate(flops=10**9, bytes_accessed=8 * 2**20, transcendentals=10**6),
    )(kh, vh, wk, ds1, after)


def body(queries, keys, values, keep_count, query_map, key_map, cotangent):
    q_rows, k_rows, v_rows, cot = queries[0], keys[0], values[0], cotangent[0]
    counts = keep_count[0]
    tokens = q_rows.shape[0]
    tiles = tokens // TILE
    peers = lax.axis_size("seq")
    me = lax.axis_index("seq")
    where = jnp.stack([me, jnp.int32(tiles)]).astype(jnp.int32)
    ring = [(a, a + 1) for a in range(peers - 1)]
    kp, vp = lax.ppermute((k_rows[tokens - TILE :], v_rows[tokens - TILE :]), "seq", ring)
    wq = jnp.swapaxes(query_map, 1, 2)
    wk = jnp.swapaxes(key_map, 1, 2)
    kh, vh, total = local_states(k_rows, v_rows, wk)
    states = sum_of_others([total[None]], "seq", False, 0)
    rest = attend(1, tiles - 1, False, counts, where, q_rows, kh, vh, kh, vh, cot, wq, wk, states)
    head = attend(0, 1, True, counts, where, q_rows, kh, vh, kp, vp, cot, wq, wk, states)
    after = sum_of_others([head[1], rest[1]], "seq", True, 1)
    gk = key_grads(kh, vh, wk, rest[1], after)
    heads, rank, width = wq.shape
    grads = sum_over_all([head[2], rest[2], head[3], rest[3], gk], ("seq", "batch"))
    grads = jnp.swapaxes(grads.reshape(2, heads, rank, width), 2, 3)
    out = jnp.concatenate([head[0], rest[0]], 0)
    return out[None], grads[0], grads[1]


def solution(mesh):
    placed = (
        P("batch", "seq", None, None),
        P("batch", "seq", None, None),
        P("batch", "seq", None, None),
        P("batch", None, None),
        P(),
        P(),
        P("batch", "seq", None, None),
    )
    return jax.shard_map(
        body,
        mesh=mesh,
        in_specs=placed,
        out_specs=(P("batch", "seq", None, None), P(), P()),
        check_vma=False,
    )
```

```python
import functools
import math

import jax
import jax.numpy as jnp
from jax import lax
from jax.experimental import pallas as pl
from jax.experimental.pallas import tpu as pltpu
from jax.sharding import PartitionSpec as P

TILE = 128
SHIFT = 1.5
LOG2E = 1.0 / math.log(2.0)
MASKED = -1e30
F32 = jnp.float32
BF16 = jnp.bfloat16
GROUP = 8
VMEM_LIMIT = 56 * 1024 * 1024


def dot_nt(a, b):
    return lax.dot_general(a, b, (((1,), (1,)), ((), ())), preferred_element_type=F32)


def dot_nn(a, b):
    return lax.dot_general(a, b, (((1,), (0,)), ((), ())), preferred_element_type=F32)


def dot_tn(a, b):
    return lax.dot_general(a, b, (((0,), (0,)), ((), ())), preferred_element_type=F32)


def by_head(x):
    return jnp.swapaxes(x, 0, 1)


def softplus(x):
    return jnp.maximum(x, 0.0) + jnp.log1p(jnp.exp(-jnp.abs(x)))


def sigmoid(x):
    return 1.0 / (1.0 + jnp.exp(-x))


def halves(x):
    top = x.astype(BF16)
    return top, (x - top.astype(F32)).astype(BF16)


def split_dot(dot, x, y):
    rows = x.shape[0]
    both = dot(jnp.concatenate(halves(x), 0), y)
    return both[:rows] + both[rows:]


def with_ones(v):
    return jnp.concatenate([v, jnp.ones(v.shape, v.dtype)], 1)


def state_kernel(k_ref, v_ref, wk_ref, kh_ref, vh_ref, total_ref, acc_ref):
    step = pl.program_id(0)
    heads = wk_ref.shape[0]
    kh_ref[...] = by_head(k_ref[...])
    vh_ref[...] = by_head(v_ref[...])

    @pl.when(step == 0)
    def _():
        acc_ref[...] = jnp.zeros_like(acc_ref)

    pre = jnp.stack([dot_nt(wk_ref[h], kh_ref[h]) for h in range(heads)], 0)
    feat = softplus(pre - SHIFT)
    for h in range(heads):
        acc_ref[h] += split_dot(dot_nn, feat[h], with_ones(vh_ref[h]))

    @pl.when(step == pl.num_programs(0) - 1)
    def _():
        total_ref[...] = acc_ref[...]


def local_states(k_rows, v_rows, wk):
    tokens, heads, width = k_rows.shape
    rank = wk.shape[1]
    row_spec = pl.BlockSpec((TILE, heads, width), lambda n: (n, 0, 0))
    head_spec = pl.BlockSpec((heads, TILE, width), lambda n: (0, n, 0))
    return pl.pallas_call(
        state_kernel,
        name="local_states",
        grid=(tokens // TILE,),
        in_specs=[row_spec, row_spec, pl.BlockSpec(wk.shape, lambda n: (0, 0, 0))],
        out_specs=[head_spec, head_spec, pl.BlockSpec((heads, rank, 2 * width), lambda n: (0, 0, 0))],
        out_shape=[
            jax.ShapeDtypeStruct((heads, tokens, width), BF16),
            jax.ShapeDtypeStruct((heads, tokens, width), BF16),
            jax.ShapeDtypeStruct((heads, rank, 2 * width), F32),
        ],
        scratch_shapes=[pltpu.VMEM((heads, rank, 2 * width), F32)],
        compiler_params=pltpu.CompilerParams(vmem_limit_bytes=VMEM_LIMIT),
        cost_estimate=pl.CostEstimate(flops=10**9, bytes_accessed=8 * 2**20, transcendentals=10**6),
    )(k_rows, v_rows, wk)


def main_kernel(
    first, halo, counts_ref, where_ref, q_ref, k_ref, v_ref, kp_ref, vp_ref, c_ref, wq_ref, wk_ref,
    states_ref, *refs,
):
    out_ref, ds_ref, gq_ref, gk_ref, qh, ch, oh, kph, vph, run = refs[-10:]
    step = pl.program_id(0)
    heads = wq_ref.shape[0]
    width = q_ref.shape[2]
    me = where_ref[0]
    tiles_dev = where_ref[1]
    factor = LOG2E / math.sqrt(width)
    qh[...] = by_head(q_ref[...])
    ch[...] = by_head(c_ref[...])
    if halo:
        kph[...] = by_head(kp_ref[...])
        vph[...] = by_head(vp_ref[...])
    prev_k = kph if halo else kp_ref
    prev_v = vph if halo else vp_ref

    @pl.when(step == 0)
    def _():
        gq_ref[...] = jnp.zeros_like(gq_ref)
        gk_ref[...] = jnp.zeros_like(gk_ref)
        run[...] = states_ref[...]

    tile = me * tiles_dev + first + step
    lane = lax.broadcasted_iota(jnp.int32, (1, TILE), 1)
    row = lax.broadcasted_iota(jnp.int32, (TILE, TILE), 0)
    col = lax.broadcasted_iota(jnp.int32, (TILE, TILE), 1)
    causal = col <= row

    def some_heads(g, carry):
        hs = [g * GROUP + i for i in range(GROUP)]
        each = range(GROUP)
        qs, ks, vs = [qh[h] for h in hs], [k_ref[h] for h in hs], [v_ref[h] for h in hs]
        kps, vps = [prev_k[h] for h in hs], [prev_v[h] for h in hs]
        own_raw = [dot_nt(qs[i], ks[i]) for i in each]
        old_raw = [dot_nt(qs[i], kps[i]) for i in each]
        pre_p = [dot_nt(wk_ref[hs[i]], kps[i]) - SHIFT for i in each]
        pre_q = [dot_nt(wq_ref[hs[i]], qs[i]) - SHIFT for i in each]
        counts = [jnp.where(tile > 0, counts_ref[h, jnp.maximum(tile - 1, 0)], 0) for h in hs]
        kept = [lane < count for count in counts]
        kept_f = [keep.astype(F32) for keep in kept]
        own = [jnp.where(causal, own_raw[i], MASKED) for i in each]
        old = [jnp.where(kept[i], old_raw[i], MASKED) for i in each]
        top = [jnp.max(jnp.maximum(own[i], old[i]), 1, keepdims=True) * factor for i in each]
        feat_p = [softplus(pre) for pre in pre_p]
        feat_q = [softplus(pre) for pre in pre_q]
        both = [
            split_dot(dot_nn, jnp.concatenate([feat_p[i], feat_p[i] * kept_f[i]], 0), with_ones(vps[i])) for i in each
        ]
        state = []
        for i in each:
            rank = feat_p[i].shape[0]
            total = run[hs[i]]
            if not halo:
                total += both[i][:rank]
                run[hs[i]] = total
            state.append(total - both[i][rank:])
        p_own = [jnp.exp2(own[i] * factor - top[i]).astype(BF16) for i in each]
        p_old = [jnp.exp2(old[i] * factor - top[i]).astype(BF16) for i in each]
        numer = [dot_nn(p_own[i], with_ones(vs[i])) + dot_nn(p_old[i], with_ones(vps[i])) for i in each]
        decay = [jnp.exp2(-t) for t in top]
        kernel = []
        for i in each:
            fq_top, fq_low = halves(feat_q[i])
            st_top, st_low = halves(state[i])
            kernel.append(
                dot_tn(jnp.concatenate([fq_top, fq_low, fq_top], 0), jnp.concatenate([st_top, st_top, st_low], 0))
            )
        g_ext = []
        for i in each:
            full = numer[i] + decay[i] * kernel[i]
            inv = 1.0 / full[:, width:]
            out = full[:, :width] * inv
            oh[hs[i]] = out.astype(BF16)
            gn = decay[i] * (ch[hs[i]].astype(F32) * inv)
            g_ext.append(jnp.concatenate([gn, gn * out], 1).astype(BF16))
        signed = [jnp.concatenate([st[:, :width], -st[:, width:]], 1) for st in state]
        d_fq = [split_dot(dot_nt, signed[i], g_ext[i]) for i in each]
        ds = [split_dot(dot_nn, feat_q[i], g_ext[i]) for i in each]
        dpre_q = [d_fq[i] * sigmoid(pre_q[i]) for i in each]
        d_fk = [
            split_dot(dot_nt, ds[i][:, :width], vps[i]) - jnp.sum(ds[i][:, width:], 1, keepdims=True) for i in each
        ]
        dpre_k = [-kept_f[i] * d_fk[i] * sigmoid(pre_p[i]) for i in each]
        gq = [split_dot(dot_nn, dpre_q[i], qs[i]) for i in each]
        gk = [split_dot(dot_nn, dpre_k[i], kps[i]) for i in each]
        for i in each:
            ds_ref[0, hs[i]] = ds[i]
            gq_ref[hs[i]] += gq[i]
            gk_ref[hs[i]] += gk[i]
        return carry

    lax.fori_loop(0, heads // GROUP, some_heads, 0)
    out_ref[...] = by_head(oh[...])


def attend(first, steps, begun, counts, where, q_rows, kh, vh, kp, vp, cot, wq, wk, states):
    tokens, heads, width = q_rows.shape
    rank = wq.shape[1]
    row_spec = pl.BlockSpec((TILE, heads, width), lambda n: (n + first, 0, 0))
    head_spec = pl.BlockSpec((heads, TILE, width), lambda n: (0, n + first, 0))
    halo = begun is not None
    if halo:
        prev_specs = [pl.BlockSpec((None, TILE, heads, width), lambda n, i=i: (i, 0, 0, 0)) for i in range(2)]
    else:
        prev_specs = [pl.BlockSpec((heads, TILE, width), lambda n: (0, n + first - 1, 0))] * 2
    whole = pl.BlockSpec((heads, rank, width), lambda n: (0, 0, 0))
    smem = pl.BlockSpec(memory_space=pltpu.SMEM)
    tile_scratch = pltpu.VMEM((heads, TILE, width), BF16)
    return pl.pallas_call(
        functools.partial(main_kernel, first, halo),
        name="attend_first" if halo else "attend_rest",
        grid=(steps,),
        in_specs=[
            smem, smem, row_spec, head_spec, head_spec, *prev_specs, row_spec, whole, whole,
            pl.BlockSpec(states.shape, lambda n: (0, 0, 0)),
        ] + [pl.BlockSpec(memory_space=pl.ANY)] * halo,
        out_specs=[
            row_spec,
            pl.BlockSpec((1, heads, rank, 2 * width), lambda n: (n, 0, 0, 0)),
            whole,
            whole,
        ],
        out_shape=[
            jax.ShapeDtypeStruct((tokens, heads, width), BF16),
            jax.ShapeDtypeStruct((steps, heads, rank, 2 * width), F32),
            jax.ShapeDtypeStruct((heads, rank, width), F32),
            jax.ShapeDtypeStruct((heads, rank, width), F32),
        ],
        scratch_shapes=[tile_scratch] * 5 + [pltpu.VMEM((heads, rank, 2 * width), F32)],
        compiler_params=pltpu.CompilerParams(vmem_limit_bytes=VMEM_LIMIT),
        cost_estimate=pl.CostEstimate(flops=10**9 * steps, bytes_accessed=steps * 4 * 2**20, transcendentals=10**6),
        input_output_aliases={11: 0} if halo else {},
    )(counts, where, q_rows, kh, vh, kp, vp, cot, wq, wk, states, *([begun] if halo else []))


def key_kernel(kh_ref, vh_ref, wk_ref, ds1_ref, after_ref, gk_ref):
    group, tokens, width = kh_ref.shape
    tiles = tokens // TILE
    each = range(group)
    pre = [dot_nt(wk_ref[h], kh_ref[h]) - SHIFT for h in each]
    grads = []
    for h in each:
        later = after_ref[h][:, :width]
        norm = after_ref[h][:, width:]
        pieces = [None] * tiles
        for n in reversed(range(tiles)):
            pieces[n] = split_dot(dot_nt, later, vh_ref[h, n * TILE : (n + 1) * TILE]) + norm
            if n:
                later += ds1_ref[n - 1, h][:, :width]
                norm -= jnp.sum(ds1_ref[n - 1, h][:, width:], 1, keepdims=True)
        grads.append(jnp.concatenate(pieces, 1))
    for h in each:
        gk_ref[h] = split_dot(dot_nn, grads[h] * sigmoid(pre[h]), kh_ref[h])


def flat_id(axes):
    index, count = 0, 1
    for axis in axes:
        index = index * lax.axis_size(axis) + lax.axis_index(axis)
        count *= lax.axis_size(axis)
    return index, count


def place(flat, axes):
    where = {}
    for axis in reversed(axes):
        size = lax.axis_size(axis)
        where[axis] = lax.rem(flat, size)
        flat = flat // size
    return where


def greet(count, me, axes):
    barrier = pltpu.get_barrier_semaphore()

    def hello(i, carry):
        pl.semaphore_signal(
            barrier, inc=1, device_id=place(lax.rem(me + i, count), axes), device_id_type=pl.DeviceIdType.MESH
        )
        return carry

    lax.fori_loop(1, count, hello, 0)
    return barrier


def others_kernel(axis, later, *refs):
    parts, (out_ref, mine, slots, send_sem, recv_sem) = refs[:-5], refs[-5:]
    heads, _, twice = out_ref.shape
    width = twice // 2
    axes = (axis,)
    me, count = flat_id(axes)
    barrier = greet(count, me, axes)
    lane = lax.broadcasted_iota(jnp.int32, (1, width), 1)
    packed = jnp.zeros(mine.shape[1:], F32)
    shape = mine.shape
    for h in range(heads):
        own = sum(part[n, h] for part in parts for n in range(part.shape[0]))
        mine[h] = own[:, :width].astype(BF16)
        norm = -jnp.sum(own[:, width:], 1, keepdims=True) if later else own[:, width:]
        packed = jnp.where(lane == h, norm, packed)
    mine[heads], mine[heads + 1] = halves(packed)
    pl.semaphore_wait(barrier, count - 1)

    def copy(sender, target):
        return pltpu.make_async_remote_copy(
            src_ref=mine,
            dst_ref=slots.at[sender],
            send_sem=send_sem.at[target],
            recv_sem=recv_sem.at[sender],
            device_id=place(target, axes),
            device_id_type=pl.DeviceIdType.MESH,
        )

    if later:
        first_to, end_to, first_from, end_from = 0, me, me + 1, count
    else:
        first_to, end_to, first_from, end_from = me + 1, count, 0, me

    def send(p, carry):
        copy(me, p).start()
        return carry

    def sent(p, carry):
        copy(me, p).wait_send()
        return carry

    def received(p, total):
        copy(p, lax.rem(me + 1, count)).wait_recv()
        return total + slots[p].astype(F32)

    lax.fori_loop(first_to, end_to, send, 0)
    total = lax.fori_loop(first_from, end_from, received, jnp.zeros(shape, F32))
    lax.fori_loop(first_to, end_to, sent, 0)
    for h in range(heads):
        norm = jnp.sum(jnp.where(lane == h, total[heads] + total[heads + 1], 0.0), 1, keepdims=True)
        out_ref[h] = jnp.concatenate([total[h], jnp.broadcast_to(norm, total[h].shape)], 1)


def sum_of_others(parts, axis, later, collective_id):
    heads, rank, twice = parts[0].shape[1:]
    count = lax.axis_size(axis)
    block = (heads + 2, rank, twice // 2)
    vmem = pl.BlockSpec(memory_space=pltpu.VMEM)
    return pl.pallas_call(
        functools.partial(others_kernel, axis, later),
        name="later_grads" if later else "earlier_states",
        in_specs=[vmem] * len(parts),
        out_specs=vmem,
        out_shape=jax.ShapeDtypeStruct((heads, rank, twice), F32),
        scratch_shapes=[
            pltpu.VMEM(block, BF16),
            pltpu.VMEM((count,) + block, BF16),
            pltpu.SemaphoreType.DMA((count,)),
            pltpu.SemaphoreType.DMA((count,)),
        ],
        compiler_params=pltpu.CompilerParams(
            collective_id=collective_id, has_side_effects=True, vmem_limit_bytes=VMEM_LIMIT
        ),
        cost_estimate=pl.CostEstimate(flops=10**7, bytes_accessed=2**20, transcendentals=0),
    )(*parts)


def reduce_kernel(axes, gq0, gq1, gk0, gk1, gk2, gq_ref, gk_ref, mine, slots, done, out_sem, in_sem, back_sem, res_sem):
    heads = gq0.shape[0]
    chunks = 2 * heads
    me, count = flat_id(axes)
    owners = min(count, chunks)
    stride, per = count // owners, chunks // owners
    barrier = greet(count, me, axes)
    mine[:heads] = gq0[...] + gq1[...]
    mine[heads:] = gk0[...] + gk1[...] + gk2[...]
    pl.semaphore_wait(barrier, count - 1)
    owner = lax.rem(me, stride) == 0
    part = me // stride

    def to_owner(o, sender):
        return pltpu.make_async_remote_copy(
            src_ref=mine.at[pl.ds(o * per, per)],
            dst_ref=slots.at[sender],
            send_sem=out_sem.at[o],
            recv_sem=in_sem.at[sender],
            device_id=place(o * stride, axes),
            device_id_type=pl.DeviceIdType.MESH,
        )

    def to_all(o, target):
        return pltpu.make_async_remote_copy(
            src_ref=done.at[pl.ds(o * per, per)],
            dst_ref=done.at[pl.ds(o * per, per)],
            send_sem=back_sem.at[target],
            recv_sem=res_sem.at[o],
            device_id=place(target, axes),
            device_id_type=pl.DeviceIdType.MESH,
        )

    def over_owners(act):
        def step(i, carry):
            o = lax.rem(part + i, owners)

            @pl.when(o * stride != me)
            def _():
                act(o)

            return carry

        lax.fori_loop(0, owners, step, 0)

    over_owners(lambda o: to_owner(o, me).start())

    @pl.when(owner)
    def _():
        def arrived(i, total):
            sender = lax.rem(me + i, count)
            to_owner(part, sender).wait_recv()
            return total + slots[sender]

        done[pl.ds(part * per, per)] = lax.fori_loop(1, count, arrived, mine[pl.ds(part * per, per)])

        def send(i, carry):
            to_all(part, lax.rem(me + i, count)).start()
            return carry

        lax.fori_loop(1, count, send, 0)

    over_owners(lambda o: to_owner(o, me).wait_send())
    over_owners(lambda o: to_all(o, lax.rem(me + 1, count)).wait_recv())

    @pl.when(owner)
    def _():
        def sent(i, carry):
            to_all(part, lax.rem(me + i, count)).wait_send()
            return carry

        lax.fori_loop(1, count, sent, 0)

    gq_ref[...] = done[:heads]
    gk_ref[...] = done[heads:]


def sum_over_all(grads, axes):
    heads, rank, width = grads[0].shape
    count = math.prod(lax.axis_size(axis) for axis in axes)
    owners = min(count, 2 * heads)
    per = 2 * heads // owners
    vmem = pl.BlockSpec(memory_space=pltpu.VMEM)
    whole = (2 * heads, rank, width)
    return pl.pallas_call(
        functools.partial(reduce_kernel, axes),
        name="sum_grads",
        in_specs=[vmem] * len(grads),
        out_specs=[vmem, vmem],
        out_shape=[jax.ShapeDtypeStruct((heads, rank, width), F32)] * 2,
        scratch_shapes=[
            pltpu.VMEM(whole, F32),
            pltpu.VMEM((count, per, rank, width), F32),
            pltpu.VMEM(whole, F32),
            pltpu.SemaphoreType.DMA((owners,)),
            pltpu.SemaphoreType.DMA((count,)),
            pltpu.SemaphoreType.DMA((count,)),
            pltpu.SemaphoreType.DMA((owners,)),
        ],
        compiler_params=pltpu.CompilerParams(collective_id=2, has_side_effects=True, vmem_limit_bytes=VMEM_LIMIT),
        cost_estimate=pl.CostEstimate(flops=10**7, bytes_accessed=2**20, transcendentals=0),
    )(*grads)


def key_grads(kh, vh, wk, ds1, after):
    heads, tokens, width = kh.shape
    rank = wk.shape[1]
    group = 4
    head_spec = pl.BlockSpec((group, tokens, width), lambda n: (n, 0, 0))
    whole = pl.BlockSpec((group, rank, width), lambda n: (n, 0, 0))
    four = pl.BlockSpec((ds1.shape[0], group, rank, 2 * width), lambda n: (0, n, 0, 0))

    return pl.pallas_call(
        key_kernel,
        name="key_grads",
        grid=(heads // group,),
        in_specs=[
            head_spec, head_spec, whole, four, pl.BlockSpec((group, rank, 2 * width), lambda n: (n, 0, 0)),
        ],
        out_specs=whole,
        out_shape=jax.ShapeDtypeStruct((heads, rank, width), F32),
        compiler_params=pltpu.CompilerParams(vmem_limit_bytes=VMEM_LIMIT),
        cost_estimate=pl.CostEstimate(flops=10**9, bytes_accessed=8 * 2**20, transcendentals=10**6),
    )(kh, vh, wk, ds1, after)


def body(queries, keys, values, keep_count, query_map, key_map, cotangent):
    q_rows, k_rows, v_rows, cot = queries[0], keys[0], values[0], cotangent[0]
    counts = keep_count[0]
    tokens = q_rows.shape[0]
    tiles = tokens // TILE
    peers = lax.axis_size("seq")
    me = lax.axis_index("seq")
    where = jnp.stack([me, jnp.int32(tiles)]).astype(jnp.int32)
    ring = [(a, a + 1) for a in range(peers - 1)]
    halo = lax.ppermute(jnp.stack([k_rows[tokens - TILE :], v_rows[tokens - TILE :]]), "seq", ring)
    wq = jnp.swapaxes(query_map, 1, 2)
    wk = jnp.swapaxes(key_map, 1, 2)
    kh, vh, total = local_states(k_rows, v_rows, wk)
    states = sum_of_others([total[None]], "seq", False, 0)
    rest = attend(1, tiles - 1, None, counts, where, q_rows, kh, vh, kh, vh, cot, wq, wk, states)
    head = attend(0, 1, rest[0], counts, where, q_rows, kh, vh, halo, halo, cot, wq, wk, states)
    after = sum_of_others([head[1], rest[1]], "seq", True, 1)
    gk = key_grads(kh, vh, wk, rest[1], after)
    grads = sum_over_all([head[2], rest[2], head[3], rest[3], gk], ("seq", "batch"))
    return head[0][None], jnp.swapaxes(grads[0], 1, 2), jnp.swapaxes(grads[1], 1, 2)


def solution(mesh):
    placed = (
        P("batch", "seq", None, None),
        P("batch", "seq", None, None),
        P("batch", "seq", None, None),
        P("batch", None, None),
        P(),
        P(),
        P("batch", "seq", None, None),
    )
    return jax.shard_map(
        body,
        mesh=mesh,
        in_specs=placed,
        out_specs=(P("batch", "seq", None, None), P(), P()),
        check_vma=False,
    )
```
